32 devices in a mesh: groups: 2 (over y), fsdp: 4 (over z), mp: 2 (over x), sub: 2 (over core).
Axes of the slice: x: 2, y: 2, z: 4, core: 2. Of those that a mesh axis runs over, the one named last changes fastest.
Arguments:
- hidden: bfloat16 [128, 36864], P(('groups', 'fsdp', 'sub'), 'mp'), parts along dimension 0, may hold values from -6 to 6
- residual: bfloat16 [128, 4608], P(('groups', 'fsdp', 'sub')), parts along dimension 0, may hold values from -6 to 6
- down_packed: int32 [4608, 4608], P('mp', 'fsdp'), may hold values from -2147483648 to 2147483646
- down_scale: bfloat16 [288, 4608], P('mp', 'fsdp'), may hold values from 0.00049972534 to 0.0019989014
- post_gain: float32 [4608], replicated, may hold values from 0.1 to 1.9
- final_gain: float32 [4608], replicated, may hold values from 0.1 to 1.9
- embed_packed: int32 [8192, 576], P(('fsdp', 'mp', 'sub')), may hold values from -2147483648 to 2147483646
- embed_scale: bfloat16 [8192, 36], P(('fsdp', 'mp', 'sub')), may hold values from 0.0059814453 to 0.029907227
- targets: int32 [128], P(('groups', 'fsdp', 'sub')), parts along dimension 0, may hold values from 0 to 8191
- loss_mask: int32 [128], P(('groups', 'fsdp', 'sub')), parts along dimension 0, may hold values 0 or 1
Outputs:
- token_loss: float32 [128], P(('groups', 'fsdp', 'sub')), parts along dimension 0
- mean_loss: float32 [2], P('groups'), parts along dimension 0
The draws below stay inside these ranges and needn't reach their ends.
There are 2 independent parts, one for each index of `groups`. The reference program is written for one: setup_inputs(seed, part) draws one part's arguments, and reference() takes and returns one part's arrays. A program takes and returns all parts, laid end to end along the dimension named above; an argument that names none is the same for every part. Nothing has to cross between parts.
Inputs may be any that keep to these rules, and one draw needn't show every extreme that they name: `down_packed`: bits 4 k to 4 k + 3 of the word in row r hold the signed code of row 8 r + k of the down projection, k = 0..7. `embed_packed`: bits 4 k to 4 k + 3 of the word in column j hold the signed code of column k * 576 + j of the embedding, k = 0..7.
All inputs are finite; a program needn't handle non-finite values. No bound on the sum of `loss_mask` on one device may be relied on, other than what follows from the above.
Results may differ from the reference program's by a relative error of at most 0.00097.
Values may be sent and summed in bfloat16 or wider, within the bound.
A program may use at most 128 MiB of HBM per device.

```python
import math
import jax
import jax.numpy as jnp
from jax import lax

D = 4608
FF = 36864
GROUP = 128
VOCAB = 8192
TOKENS = 64
N_MP = 2


def with_ends(entries, stream_key, smallest, largest):
    shape = entries.shape
    spot = [jax.random.randint(jax.random.fold_in(stream_key, axis), (), 0, shape[axis]) for axis in range(len(shape))]
    entries = entries.at[tuple(spot)].set(smallest)
    longest = shape.index(max(shape))
    spot[longest] = (spot[longest] + 1) % shape[longest]
    return entries.at[tuple(spot)].set(largest)


def levels(own_key, extent, pieces, smallest, top_value):
    gain, own = 1.0, jax.random.fold_in(own_key, 6)
    for dim, blocks in pieces:
        steps = jnp.exp(jax.random.uniform(jax.random.fold_in(own, dim), (blocks,), jnp.float32, smallest / len(pieces), top_value / len(pieces)))
        gain = gain * jnp.repeat(steps, extent[dim] // blocks).reshape([-1 if axis == dim else 1 for axis in range(len(extent))])
    return gain


def scatter_about(rng, extent, scale, reach, shards=(), held_as=jnp.bfloat16):
    gain = levels(rng, extent, shards, -0.22, 0.18) if shards else 1.0
    drawn = jax.random.normal(rng, extent, jnp.float32) * scale * gain
    return jnp.minimum(jnp.maximum(drawn, -reach), reach).astype(held_as)


def setup_inputs(seed: int = 0, part: int = 0) -> dict:
    streams_of = jax.random.split(jax.random.key(seed), 11)
    part_keys = jax.random.split(jax.random.fold_in(streams_of[10], part), 11)
    return {
        "hidden": scatter_about(part_keys[0], (TOKENS, FF), 1.0, 6.0, ((0, 8), (1, 2))),
        "residual": scatter_about(part_keys[1], (TOKENS, D), 1.0, 6.0, ((0, 8),)),
        "down_packed": with_ends(jax.random.randint(streams_of[2], (FF // 8, D), -2147483648, 2147483647), jax.random.fold_in(streams_of[2], 1), -2147483648, 2147483646).astype(jnp.int32),
        "down_scale": jnp.clip(jnp.exp(math.log(0.0019989014) - 1.3862944 * jax.random.uniform(streams_of[3], (FF // GROUP, D), jnp.float32) ** levels(streams_of[3], (FF // GROUP, D), ((0, 2), (1, 4)), -0.2, 0.2)), 0.00049972534, 0.0019989014).astype(jnp.bfloat16),
        "post_gain": jnp.clip(1.0 + 0.18 * jax.random.normal(streams_of[4], (D,), jnp.float32), 0.1, 1.9),
        "final_gain": jnp.clip(1.0 + 0.18 * jax.random.normal(streams_of[5], (D,), jnp.float32), 0.1, 1.9),
        "embed_packed": with_ends(jax.random.randint(streams_of[6], (VOCAB, D // 8), -2147483648, 2147483647), jax.random.fold_in(streams_of[6], 1), -2147483648, 2147483646).astype(jnp.int32),
        "embed_scale": jnp.clip(jnp.exp(math.log(0.029907227) - 1.609438 * jax.random.uniform(streams_of[7], (VOCAB, D // GROUP), jnp.float32) ** levels(streams_of[7], (VOCAB, D // GROUP), ((0, 16),), -0.2, 0.2)), 0.0059814453, 0.029907227).astype(jnp.bfloat16),
        "targets": with_ends(jax.random.randint(part_keys[8], (TOKENS,), 0, VOCAB), jax.random.fold_in(part_keys[8], 1), 0, VOCAB - 1).astype(jnp.int32),
        "loss_mask": with_ends((jax.random.randint(part_keys[9], (TOKENS,), 0, 4) < 3).astype(jnp.int32), jax.random.fold_in(part_keys[9], 1), 0, 1),
    }


EPS = 1e-06
CAP = 30.0

def signed_planes(words):
    shifts = (28 - 4 * jnp.arange(8, dtype=jnp.int32))[None, :, None]
    lifted = jnp.left_shift(words[:, None, :], shifts)
    return jnp.right_shift(lifted, 28)

def dequant_down(words, scales):
    cols = words.shape[1]
    codes = signed_planes(words).astype(jnp.bfloat16)
    grouped = codes.reshape(scales.shape[0], -1, cols) * scales[:, None, :]
    return grouped.reshape(-1, cols)

def dequant_embed(words, scales):
    rows = words.shape[0]
    codes = signed_planes(words).astype(jnp.bfloat16)
    grouped = codes.reshape(rows, scales.shape[1], -1) * scales[:, :, None]
    return grouped.reshape(rows, -1)

def reference(hidden, residual, down_packed, down_scale, post_gain, final_gain, embed_packed, embed_scale, targets, loss_mask):
    block = FF // N_MP
    ffn = jnp.zeros((TOKENS, D), jnp.float32)
    for b in range(N_MP):
        weight = dequant_down(down_packed[b * block // 8:(b + 1) * block // 8], down_scale[b * block // GROUP:(b + 1) * block // GROUP])
        ffn = ffn + jnp.dot(hidden[:, b * block:(b + 1) * block], weight, preferred_element_type=jnp.float32)
    normed = ffn * lax.rsqrt(lax.optimization_barrier(jnp.mean(ffn * ffn, axis=-1, keepdims=True)) + EPS) * post_gain
    stream = residual.astype(jnp.float32) + normed
    states = (stream * lax.rsqrt(lax.optimization_barrier(jnp.mean(stream * stream, axis=-1, keepdims=True)) + EPS) * final_gain).astype(jnp.bfloat16)
    vrows = VOCAB // N_MP
    exp_sums = jnp.zeros((TOKENS,), jnp.float32)
    target_logits = jnp.zeros((TOKENS,), jnp.float32)
    for b in range(N_MP):
        embed = dequant_embed(embed_packed[b * vrows:(b + 1) * vrows], embed_scale[b * vrows:(b + 1) * vrows])
        logits = lax.dot_general(states, embed, (((1,), (1,)), ((), ())), preferred_element_type=jnp.float32)
        capped = CAP * jnp.tanh(logits / CAP)
        exp_sums = exp_sums + lax.optimization_barrier(jnp.sum(jnp.exp(capped), axis=1))
        ids = b * vrows + jnp.arange(vrows, dtype=jnp.int32)
        hits = targets[:, None] == ids[None, :]
        target_logits = target_logits + lax.optimization_barrier(jnp.sum(jnp.where(hits, capped, 0.0), axis=1))
    weights = loss_mask.astype(jnp.float32)
    token_loss = weights * (jnp.log(exp_sums) - target_logits)
    mean_loss = jnp.sum(token_loss) / jnp.maximum(jnp.sum(weights), 1.0)
    return (token_loss, mean_loss.reshape(1))
```

```python
import functools

import jax
import jax.numpy as jnp
from jax import lax
from jax.experimental import pallas as pl
from jax.experimental.pallas import tpu as pltpu
from jax.sharding import PartitionSpec as P

EPS = 1e-06
CAP = 30.0
MESH = pl.DeviceIdType.MESH
PLANES = 8
EARLY = 0.6


def remote(src, dst, send, recv, f, m, s):
    return pltpu.make_async_remote_copy(
        src_ref=src,
        dst_ref=dst,
        send_sem=send,
        recv_sem=recv,
        device_id={"fsdp": f, "mp": m, "sub": s},
        device_id_type=MESH,
    )


def kernel(
    nf, nm, hidden, residual, words_hbm, scale, post_gain, final_gain, embed_hbm, embed_scale, info,
    out, words, scale_f, weight, perm, pair, gathered, own_acc, acc_in, mid, mid_in, red, cols_in,
    embed_words, embed, states, infos, sums,
    local_sem, pair_send, pair_recv, ring_send, ring_recv, info_send, info_recv,
    acc_sem, mid_send, mid_recv, col_send, col_recv, st_send, st_recv, fwd_send, fwd_recv,
    sum_send, sum_recv,
):
    f, m, s = lax.axis_index("fsdp"), lax.axis_index("mp"), lax.axis_index("sub")
    n = nf * nm * 2
    me = (f * nm + m) * 2 + s
    tok = hidden.shape[0]
    half_rows, cols = words.shape
    half_k = half_rows * PLANES
    total = tok * 2 * nf

    def where_is(q):
        return q // (2 * nm), (q // 2) % nm, q % 2

    load_words = pltpu.make_async_copy(
        words_hbm.at[pl.ds(pl.multiple_of(s * half_rows, 8), half_rows)], words, local_sem.at[0]
    )
    load_words.start()
    load_embed = pltpu.make_async_copy(embed_hbm, embed_words, local_sem.at[1])
    load_embed.start()

    barrier = pltpu.get_barrier_semaphore()
    for d in range(1, n):
        pf, pm, ps = where_is(lax.rem(me + d, n))
        pl.semaphore_signal(
            barrier, inc=1, device_id={"fsdp": pf, "mp": pm, "sub": ps}, device_id_type=MESH
        )

    width = perm.shape[0]
    q = width // PLANES
    step_rows = 128 if width % 128 == 0 else width

    def build(i, carry):
        start = pl.multiple_of(i * step_rows, step_rows)
        row = lax.broadcasted_iota(jnp.int32, (step_rows, width), 0) + start
        col = lax.broadcasted_iota(jnp.int32, (step_rows, width), 1)
        plane = sum(((col >= q * k).astype(jnp.int32) for k in range(1, PLANES)), jnp.zeros_like(col))
        source = (col - plane * q) * PLANES + plane
        perm[pl.ds(start, step_rows), :] = jnp.where(row == source, 1.0, 0.0).astype(jnp.bfloat16)
        return carry

    lax.fori_loop(0, width // step_rows, build, 0)
    scale_f[...] = scale[...].astype(jnp.float32)
    pair[s] = hidden[:, pl.ds(pl.multiple_of(s * half_k, 128), half_k)]
    infos[me] = info[...]

    pl.semaphore_wait(barrier, n - 1)

    swap = remote(
        hidden.at[:, pl.ds(pl.multiple_of((1 - s) * half_k, 128), half_k)],
        pair.at[s], pair_send, pair_recv, f, m, 1 - s,
    )
    swap.start()
    swap.wait_recv()

    both = pair[...].astype(jnp.float32).reshape(2 * tok, half_k)
    chunks = half_k // width
    stacked = jnp.concatenate(
        [both[:, c * width:(c + 1) * width] for c in range(chunks)], axis=0
    ).astype(jnp.bfloat16)
    ordered = jnp.dot(stacked, perm[...], preferred_element_type=jnp.float32).astype(jnp.bfloat16)
    for c in range(chunks):
        for k in range(PLANES):
            gathered[f, k, :, c * q:(c + 1) * q] = ordered[
                c * 2 * tok:(c + 1) * 2 * tok, k * q:(k + 1) * q
            ]

    far = nf // 2
    low, high = list(range(4)), list(range(4, 8))
    orders = (low + high, high + low)
    last = (low, high)
    pending = []
    waited = set()

    def block_at(way, j):
        return lax.rem(f - j + nf, nf) if way == 0 else lax.rem(f + j, nf)

    def hop(way, j, p):
        slot = block_at(way, j - 1)
        target = lax.rem(f + 1, nf) if way == 0 else lax.rem(f + nf - 1, nf)
        return remote(
            gathered.at[slot, p], gathered.at[slot, p], ring_send.at[way, j - 1, p],
            ring_recv.at[slot, p], target, m, s,
        )

    def send_hop(way, j, p):
        if j < far or p in last[way]:
            copy = hop(way, j, p)
            copy.start()
            pending.append(copy)

    def arrive(way, j, p):
        if (way, j, p) in waited or not (j < far or p in last[way]):
            return
        waited.add((way, j, p))
        slot = block_at(way, j)
        remote(
            gathered.at[slot, p], gathered.at[slot, p], ring_send.at[way, j - 1, p],
            ring_recv.at[slot, p], f, m, 1 - s,
        ).wait_recv()

    if nf > 1:
        for i in range(PLANES):
            for way in (0, 1):
                send_hop(way, 1, orders[way][i])

    for d in range(1, n):
        peer = lax.rem(me + d, n)
        pf, pm, ps = where_is(peer)
        copy = remote(info, infos.at[me], info_send.at[d], info_recv.at[me], pf, pm, ps)
        copy.start()
        pending.append(copy)

    load_words.wait()
    per = half_rows // (scale.shape[0] // 2)
    groups = half_rows // per

    def dequant(i, carry):
        start = pl.multiple_of(i * per, per)
        w = words[pl.ds(start, per), :]
        sc = scale_f[pl.ds(s * groups + i, 1), :]
        for k in range(PLANES):
            code = jnp.right_shift(jnp.left_shift(w, 28 - 4 * k), 28) if k < 7 else jnp.right_shift(w, 28)
            weight[k, pl.ds(start, per), :] = (code.astype(jnp.float32) * sc).astype(jnp.bfloat16)
        return carry

    early = int(groups * EARLY)
    lax.fori_loop(0, early, dequant, 0)
    for j in range(1, far):
        for i in range(PLANES):
            for way in (0, 1):
                p = orders[way][i]
                if j + 1 < far or p in last[way]:
                    arrive(way, j, p)
                    send_hop(way, j + 1, p)
    lax.fori_loop(early, groups, dequant, 0)

    load_embed.wait()
    vocab, packed = embed_words.shape
    erows = 32
    tiles = 2 * packed // 128

    def dequant_embed(i, carry):
        start = pl.multiple_of(i * erows, erows)
        w = embed_words[pl.ds(start, erows), :]
        side = jnp.concatenate([w, w], axis=1)
        es = embed_scale[pl.ds(start, erows), :].astype(jnp.float32)
        lane = lax.broadcasted_iota(jnp.int32, (erows, 128), 1)
        for kk in range(PLANES // 2):
            for t in range(tiles):
                x = side[:, t * 128:(t + 1) * 128]
                a = 28 - 8 * kk
                if (t + 1) * 128 <= packed:
                    x = jnp.left_shift(x, a)
                elif t * 128 >= packed:
                    x = jnp.left_shift(x, a - 4)
                else:
                    x = jnp.left_shift(x, jnp.where(lane < packed - t * 128, a, a - 4))
                g = kk * tiles + t
                embed[pl.ds(start, erows), g * 128:(g + 1) * 128] = (
                    jnp.right_shift(x, 28).astype(jnp.float32) * es[:, g:g + 1]
                ).astype(jnp.bfloat16)
        return carry

    lax.fori_loop(0, vocab // erows, dequant_embed, 0)

    acc = jnp.zeros((total, cols), jnp.float32)
    for p in (0, 4, 1, 5, 2, 6, 3, 7):
        for j in range(1, far + 1):
            for way in (0, 1):
                arrive(way, j, p)
        lhs = gathered[:, p].reshape(total, half_rows)
        acc = acc + jnp.dot(lhs, weight[p], preferred_element_type=jnp.float32)

    for b in range(nf):
        for h in (0, 1):
            r = (2 * b + h) * tok
            own_acc[h, b] = acc[r:r + tok]

    swap_acc = remote(own_acc.at[1 - s], acc_in, acc_sem.at[0], acc_sem.at[1], f, m, 1 - s)
    swap_acc.start()
    swap_acc.wait_recv()
    for b in range(nf):
        mid[b % nm, b // nm] = own_acc[s, b] + acc_in[b]
    for d in range(1, nm):
        pm = lax.rem(m + d, nm)
        copy = remote(mid.at[pm], mid_in.at[m], mid_send.at[d], mid_recv.at[m], f, pm, s)
        copy.start()
        pending.append(copy)
    part = mid[m]
    for d in range(1, nm):
        pm = lax.rem(m + d, nm)
        remote(mid.at[m], mid_in.at[pm], mid_send.at[0], mid_recv.at[pm], f, pm, s).wait_recv()
        part = part + mid_in[pm]
    red[...] = part

    def to_owner(j):
        target = j * nm + m
        return target, remote(
            red.at[j], cols_in.at[f], col_send.at[j], col_recv.at[f], target, m, s
        )

    for j in range(nf // nm):
        target, copy = to_owner(j)

        @pl.when(target != f)
        def _():
            copy.start()

        @pl.when(target == f)
        def _():
            cols_in[f] = red[j]

    owner = lax.rem(f, nm) == m

    def state_sends():
        copies = []
        for df in range(nf):
            for dm in range(nm):
                if df or dm:
                    copies.append(remote(
                        states.at[f, s], states.at[f, s], st_send.at[df * nm + dm], st_recv.at[f],
                        lax.rem(f + df, nf), lax.rem(m + dm, nm), s,
                    ))
        return copies

    width_d = nf * cols

    @pl.when(owner)
    def _():
        for d in range(1, nf):
            src = lax.rem(f + d, nf)
            remote(
                red.at[0], cols_in.at[src], col_send.at[0], col_recv.at[src], src, m, s
            ).wait_recv()
        ffn = jnp.concatenate([cols_in[b] for b in range(nf)], axis=1)
        inv = lax.rsqrt(jnp.sum(ffn * ffn, axis=1, keepdims=True) / width_d + EPS)
        stream = residual[...].astype(jnp.float32) + ffn * inv * post_gain[...]
        inv2 = lax.rsqrt(jnp.sum(stream * stream, axis=1, keepdims=True) / width_d + EPS)
        states[f, s] = (stream * inv2 * final_gain[...]).astype(jnp.bfloat16)
        for copy in state_sends():
            copy.start()

    def forward(b):
        return remote(
            states.at[b, s], states.at[b, s], fwd_send.at[b], fwd_recv.at[b], f, m, 1 - s
        )

    for d in range(nf):
        b = lax.rem(f + d, nf)
        got = remote(
            states.at[b, s], states.at[b, s], st_send.at[0], st_recv.at[b], f, m, 1 - s
        )
        if d == 0:
            @pl.when(jnp.logical_not(owner))
            def _():
                got.wait_recv()
        else:
            got.wait_recv()
        copy = forward(b)
        copy.start()
        pending.append(copy)
    for b in range(nf):
        remote(
            states.at[b, 1 - s], states.at[b, 1 - s], fwd_send.at[b], fwd_recv.at[b], f, m, 1 - s
        ).wait_recv()
    for d in range(1, n):
        src = lax.rem(me + n - d, n)
        remote(
            info, infos.at[src], info_send.at[d], info_recv.at[src], f, m, 1 - s
        ).wait_recv()

    all_states = states[...].astype(jnp.float32).reshape(total, width_d).astype(jnp.bfloat16)
    logits = lax.dot_general(
        all_states, embed[...], (((1,), (1,)), ((), ())), preferred_element_type=jnp.float32
    )
    capped = CAP * jnp.tanh(logits / CAP)
    rows = jnp.concatenate(
        [infos[b * nm * 2 + h] for b in range(nf) for h in (0, 1)], axis=0
    )
    ids = me * vocab + lax.broadcasted_iota(jnp.int32, (total, vocab), 1)
    hits = rows[:, 0:1] == ids
    e = jnp.sum(jnp.exp(capped), axis=1, keepdims=True)
    t = jnp.sum(jnp.where(hits, capped, 0.0), axis=1, keepdims=True)
    counted = rows[:, 64:65].astype(jnp.float32)
    lane = lax.broadcasted_iota(jnp.int32, (total, 128), 1)
    table = jnp.where(lane == 0, e, jnp.where(lane == 1, t, jnp.where(lane == 2, counted, 0.0)))
    pad = sums.shape[2]
    if pad > total:
        table = jnp.concatenate([table, jnp.zeros((pad - total, 128), jnp.float32)], axis=0)
    mine = jnp.transpose(table)[0:8, :]
    sums[me] = mine
    for d in range(1, n):
        pf, pm, ps = where_is(lax.rem(me + d, n))
        copy = remote(sums.at[me], sums.at[me], sum_send.at[d], sum_recv.at[me], pf, pm, ps)
        copy.start()
        pending.append(copy)
    for d in range(1, n):
        src = lax.rem(me + n - d, n)
        remote(
            sums.at[src], sums.at[src], sum_send.at[d], sum_recv.at[src], f, m, 1 - s
        ).wait_recv()
    added = jnp.sum(sums[...], axis=0)
    weights = mine[2:3, :]
    spot = lax.broadcasted_iota(jnp.int32, (1, pad), 1)
    exp_sums = jnp.where(spot < total, added[0:1, :], 1.0)
    losses = weights * (jnp.log(exp_sums) - added[1:2, :])
    mean = jnp.sum(losses, axis=1, keepdims=True) / jnp.maximum(
        jnp.sum(weights, axis=1, keepdims=True), 1.0
    )
    row = lax.broadcasted_iota(jnp.int32, (8, pad), 0)
    out[...] = jnp.where(row == 0, losses, mean)

    swap.wait_send()
    swap_acc.wait_send()
    for copy in pending:
        copy.wait_send()
    for j in range(nf // nm):
        target, copy = to_owner(j)

        @pl.when(target != f)
        def _():
            copy.wait_send()

    @pl.when(owner)
    def _():
        for copy in state_sends():
            copy.wait_send()


def on_device(
    nf, nm, hidden, residual, down_packed, down_scale, post_gain, final_gain, embed_packed, embed_scale,
    targets, loss_mask,
):
    tok, width_d = residual.shape
    rows, cols = down_packed.shape
    vocab, packed = embed_packed.shape
    half = rows // 2
    n = nf * nm * 2
    total = tok * 2 * nf
    pad = -(-total // 128) * 128
    chunk = PLANES * (128 if half % 128 == 0 else half)
    info = jnp.concatenate(
        [jnp.broadcast_to(targets[:, None], (tok, 64)), jnp.broadcast_to(loss_mask[:, None], (tok, 64))],
        axis=1,
    )
    vm = pl.BlockSpec(memory_space=pltpu.VMEM)
    hbm = pl.BlockSpec(memory_space=pl.ANY)
    dma = pltpu.SemaphoreType.DMA
    bf16, f32, i32 = jnp.bfloat16, jnp.float32, jnp.int32
    table = pl.pallas_call(
        functools.partial(kernel, nf, nm),
        out_shape=jax.ShapeDtypeStruct((8, pad), f32),
        in_specs=[vm, vm, hbm, vm, vm, vm, hbm, vm, vm],
        out_specs=vm,
        scratch_shapes=[
            pltpu.VMEM((half, cols), i32),
            pltpu.VMEM(down_scale.shape, f32),
            pltpu.VMEM((PLANES, half, cols), bf16),
            pltpu.VMEM((chunk, chunk), bf16),
            pltpu.VMEM((2, tok, half * PLANES), bf16),
            pltpu.VMEM((nf, PLANES, 2 * tok, half), bf16),
            pltpu.VMEM((2, nf, tok, cols), f32),
            pltpu.VMEM((nf, tok, cols), f32),
            pltpu.VMEM((nm, nf // nm, tok, cols), f32),
            pltpu.VMEM((nm, nf // nm, tok, cols), f32),
            pltpu.VMEM((nf // nm, tok, cols), f32),
            pltpu.VMEM((nf, tok, cols), f32),
            pltpu.VMEM((vocab, packed), i32),
            pltpu.VMEM((vocab, width_d), bf16),
            pltpu.VMEM((nf, 2, tok, width_d), bf16),
            pltpu.VMEM((n, tok, 128), i32),
            pltpu.VMEM((n, 8, pad), f32),
            dma((2,)),
            dma, dma,
            dma((2, max(nf // 2, 1), PLANES)), dma((nf, PLANES)),
            dma((n,)), dma((n,)),
            dma((2,)),
            dma((nm,)), dma((nm,)),
            dma((nf // nm,)), dma((nf,)),
            dma((nf * nm,)), dma((nf,)),
            dma((nf,)), dma((nf,)),
            dma((n,)), dma((n,)),
        ],
        compiler_params=pltpu.CompilerParams(
            collective_id=0, has_side_effects=True, vmem_limit_bytes=62 * 1024 * 1024
        ),
    )(
        hidden, residual, down_packed, down_scale, post_gain[None, :], final_gain[None, :],
        embed_packed, embed_scale, info,
    )
    start = (lax.axis_index("fsdp") * 2 + lax.axis_index("sub")) * tok
    return lax.dynamic_slice(table[0], (start,), (tok,)), table[1, 0:1]


def solution(mesh):
    nf, nm = mesh.shape["fsdp"], mesh.shape["mp"]
    return jax.shard_map(
        functools.partial(on_device, nf, nm),
        mesh=mesh,
        in_specs=(
            P(("groups", "fsdp", "sub"), "mp"),
            P(("groups", "fsdp", "sub"), None),
            P("mp", "fsdp"),
            P("mp", "fsdp"),
            P(),
            P(),
            P(("fsdp", "mp", "sub"), None),
            P(("fsdp", "mp", "sub"), None),
            P(("groups", "fsdp", "sub")),
            P(("groups", "fsdp", "sub")),
        ),
        out_specs=(P(("groups", "fsdp", "sub")), P("groups")),
        check_vma=False,
    )
```

```python
import functools

import jax
import jax.numpy as jnp
from jax import lax
from jax.experimental import pallas as pl
from jax.experimental.pallas import tpu as pltpu
from jax.sharding import PartitionSpec as P

EPS = 1e-06
CAP = 30.0
MESH = pl.DeviceIdType.MESH
PLANES = 8
EARLY = 0.6


def remote(src, dst, send, recv, f, m, s):
    return pltpu.make_async_remote_copy(
        src_ref=src,
        dst_ref=dst,
        send_sem=send,
        recv_sem=recv,
        device_id={"fsdp": f, "mp": m, "sub": s},
        device_id_type=MESH,
    )


def kernel(
    nf, nm, hidden, residual, words_hbm, scale, post_gain, final_gain, embed_hbm, embed_scale, targets, mask,
    out, mean_out, words, scale_f, weight, perm, pair, gathered, own_acc, acc_in, mid, mid_in, red, cols_in,
    embed_words, embed_f, embed, states, info, infos, sums,
    local_sem, pair_send, pair_recv, ring_send, ring_recv, info_send, info_recv,
    acc_sem, mid_send, mid_recv, col_send, col_recv, st_send, st_recv, fwd_send, fwd_recv,
    sum_send, sum_recv,
):
    f, m, s = lax.axis_index("fsdp"), lax.axis_index("mp"), lax.axis_index("sub")
    n = nf * nm * 2
    me = (f * nm + m) * 2 + s
    tok = hidden.shape[0]
    half_rows, cols = words.shape
    half_k = half_rows * PLANES
    total = tok * 2 * nf

    def where_is(q):
        return q // (2 * nm), (q // 2) % nm, q % 2

    load_words = pltpu.make_async_copy(
        words_hbm.at[pl.ds(pl.multiple_of(s * half_rows, 8), half_rows)], words, local_sem.at[0]
    )
    load_words.start()
    load_embed = pltpu.make_async_copy(embed_hbm, embed_words, local_sem.at[1])
    load_embed.start()

    barrier = pltpu.get_barrier_semaphore()
    for d in range(1, n):
        pf, pm, ps = where_is(lax.rem(me + d, n))
        pl.semaphore_signal(
            barrier, inc=1, device_id={"fsdp": pf, "mp": pm, "sub": ps}, device_id_type=MESH
        )

    width = perm.shape[0]
    q = width // PLANES
    step_rows = 128 if width % 128 == 0 else width

    def build(i, carry):
        start = pl.multiple_of(i * step_rows, step_rows)
        row = lax.broadcasted_iota(jnp.int32, (step_rows, width), 0) + start
        col = lax.broadcasted_iota(jnp.int32, (step_rows, width), 1)
        plane = sum(((col >= q * k).astype(jnp.int32) for k in range(1, PLANES)), jnp.zeros_like(col))
        source = (col - plane * q) * PLANES + plane
        perm[pl.ds(start, step_rows), :] = jnp.where(row == source, 1.0, 0.0).astype(jnp.bfloat16)
        return carry

    lax.fori_loop(0, width // step_rows, build, 0)
    scale_f[...] = scale[...].astype(jnp.float32)
    pair[s] = hidden[:, pl.ds(pl.multiple_of(s * half_k, 128), half_k)]
    embed_f[...] = embed_scale[...].astype(jnp.float32)
    token = lax.broadcasted_iota(jnp.int32, (tok, 128), 0)
    side = lax.broadcasted_iota(jnp.int32, (tok, 128), 1)
    entry = jnp.zeros((tok, 128), jnp.int32)
    for i in range(tok):
        entry = jnp.where(token == i, jnp.where(side < 64, targets[i], mask[i]), entry)
    info[...] = entry
    infos[me] = entry

    pl.semaphore_wait(barrier, n - 1)

    swap = remote(
        hidden.at[:, pl.ds(pl.multiple_of((1 - s) * half_k, 128), half_k)],
        pair.at[s], pair_send, pair_recv, f, m, 1 - s,
    )
    swap.start()
    swap.wait_recv()

    both = pair[...].astype(jnp.float32).reshape(2 * tok, half_k)
    chunks = half_k // width
    stacked = jnp.concatenate(
        [both[:, c * width:(c + 1) * width] for c in range(chunks)], axis=0
    ).astype(jnp.bfloat16)
    ordered = jnp.dot(stacked, perm[...], preferred_element_type=jnp.float32).astype(jnp.bfloat16)
    for c in range(chunks):
        for k in range(PLANES):
            gathered[f, k, :, c * q:(c + 1) * q] = ordered[
                c * 2 * tok:(c + 1) * 2 * tok, k * q:(k + 1) * q
            ]

    far = nf // 2
    low, high = list(range(4)), list(range(4, 8))
    orders = (low + high, high + low)
    last = (low, high)
    pending = []
    waited = set()

    def block_at(way, j):
        return lax.rem(f - j + nf, nf) if way == 0 else lax.rem(f + j, nf)

    def hop(way, j, p):
        slot = block_at(way, j - 1)
        target = lax.rem(f + 1, nf) if way == 0 else lax.rem(f + nf - 1, nf)
        return remote(
            gathered.at[slot, p], gathered.at[slot, p], ring_send.at[way, j - 1, p],
            ring_recv.at[slot, p], target, m, s,
        )

    def send_hop(way, j, p):
        if j < far or p in last[way]:
            copy = hop(way, j, p)
            copy.start()
            pending.append(copy)

    def arrive(way, j, p):
        if (way, j, p) in waited or not (j < far or p in last[way]):
            return
        waited.add((way, j, p))
        slot = block_at(way, j)
        remote(
            gathered.at[slot, p], gathered.at[slot, p], ring_send.at[way, j - 1, p],
            ring_recv.at[slot, p], f, m, 1 - s,
        ).wait_recv()

    if nf > 1:
        for i in range(PLANES):
            for way in (0, 1):
                send_hop(way, 1, orders[way][i])

    for d in range(1, n):
        peer = lax.rem(me + d, n)
        pf, pm, ps = where_is(peer)
        copy = remote(info, infos.at[me], info_send.at[d], info_recv.at[me], pf, pm, ps)
        copy.start()
        pending.append(copy)

    load_words.wait()
    per = half_rows // (scale.shape[0] // 2)
    groups = half_rows // per

    def dequant(i, carry):
        start = pl.multiple_of(i * per, per)
        w = words[pl.ds(start, per), :]
        sc = scale_f[pl.ds(s * groups + i, 1), :]
        for k in range(PLANES):
            code = jnp.right_shift(jnp.left_shift(w, 28 - 4 * k), 28) if k < 7 else jnp.right_shift(w, 28)
            weight[k, pl.ds(start, per), :] = (code.astype(jnp.float32) * sc).astype(jnp.bfloat16)
        return carry

    early = int(groups * EARLY)
    lax.fori_loop(0, early, dequant, 0)
    for j in range(1, far):
        for i in range(PLANES):
            for way in (0, 1):
                p = orders[way][i]
                if j + 1 < far or p in last[way]:
                    arrive(way, j, p)
                    send_hop(way, j + 1, p)
    lax.fori_loop(early, groups, dequant, 0)

    load_embed.wait()
    packed, vocab = embed_words.shape
    span = packed * PLANES // embed_f.shape[0]
    step = 32
    blocks = packed // step

    def dequant_embed(i, carry):
        w = embed_words[pl.ds(pl.multiple_of(i * step, step), step), :]
        for k in range(PLANES):
            code = jnp.right_shift(jnp.left_shift(w, 28 - 4 * k), 28) if k < 7 else jnp.right_shift(w, 28)
            sc = embed_f[pl.ds((k * packed + i * step) // span, 1), :]
            embed[pl.ds(pl.multiple_of(k * packed + i * step, step), step), :] = (
                code.astype(jnp.float32) * sc
            ).astype(jnp.bfloat16)
        return carry

    lax.fori_loop(0, blocks, dequant_embed, 0)

    acc = jnp.zeros((total, cols), jnp.float32)
    for p in (0, 4, 1, 5, 2, 6, 3, 7):
        for j in range(1, far + 1):
            for way in (0, 1):
                arrive(way, j, p)
        lhs = gathered[:, p].reshape(total, half_rows)
        acc = acc + jnp.dot(lhs, weight[p], preferred_element_type=jnp.float32)

    for b in range(nf):
        for h in (0, 1):
            r = (2 * b + h) * tok
            own_acc[h, b] = acc[r:r + tok]

    swap_acc = remote(own_acc.at[1 - s], acc_in, acc_sem.at[0], acc_sem.at[1], f, m, 1 - s)
    swap_acc.start()
    swap_acc.wait_recv()
    for b in range(nf):
        mid[b % nm, b // nm] = own_acc[s, b] + acc_in[b]
    for d in range(1, nm):
        pm = lax.rem(m + d, nm)
        copy = remote(mid.at[pm], mid_in.at[m], mid_send.at[d], mid_recv.at[m], f, pm, s)
        copy.start()
        pending.append(copy)
    part = mid[m]
    for d in range(1, nm):
        pm = lax.rem(m + d, nm)
        remote(mid.at[m], mid_in.at[pm], mid_send.at[0], mid_recv.at[pm], f, pm, s).wait_recv()
        part = part + mid_in[pm]
    red[...] = part

    def to_owner(j):
        target = j * nm + m
        return target, remote(
            red.at[j], cols_in.at[f], col_send.at[j], col_recv.at[f], target, m, s
        )

    for j in range(nf // nm):
        target, copy = to_owner(j)

        @pl.when(target != f)
        def _():
            copy.start()

        @pl.when(target == f)
        def _():
            cols_in[f] = red[j]

    owner = lax.rem(f, nm) == m

    def state_sends():
        copies = []
        for df in range(nf):
            for dm in range(nm):
                if df or dm:
                    copies.append(remote(
                        states.at[f, s], states.at[f, s], st_send.at[df * nm + dm], st_recv.at[f],
                        lax.rem(f + df, nf), lax.rem(m + dm, nm), s,
                    ))
        return copies

    width_d = nf * cols

    @pl.when(owner)
    def _():
        for d in range(1, nf):
            src = lax.rem(f + d, nf)
            remote(
                red.at[0], cols_in.at[src], col_send.at[0], col_recv.at[src], src, m, s
            ).wait_recv()
        ffn = jnp.concatenate([cols_in[b] for b in range(nf)], axis=1)
        inv = lax.rsqrt(jnp.sum(ffn * ffn, axis=1, keepdims=True) / width_d + EPS)
        stream = residual[...].astype(jnp.float32) + ffn * inv * post_gain[...].reshape(1, width_d)
        inv2 = lax.rsqrt(jnp.sum(stream * stream, axis=1, keepdims=True) / width_d + EPS)
        states[f, s] = (stream * inv2 * final_gain[...].reshape(1, width_d)).astype(jnp.bfloat16)
        for copy in state_sends():
            copy.start()

    def forward(b):
        return remote(
            states.at[b, s], states.at[b, s], fwd_send.at[b], fwd_recv.at[b], f, m, 1 - s
        )

    for d in range(nf):
        b = lax.rem(f + d, nf)
        got = remote(
            states.at[b, s], states.at[b, s], st_send.at[0], st_recv.at[b], f, m, 1 - s
        )
        if d == 0:
            @pl.when(jnp.logical_not(owner))
            def _():
                got.wait_recv()
        else:
            got.wait_recv()
        copy = forward(b)
        copy.start()
        pending.append(copy)
    for b in range(nf):
        remote(
            states.at[b, 1 - s], states.at[b, 1 - s], fwd_send.at[b], fwd_recv.at[b], f, m, 1 - s
        ).wait_recv()
    for d in range(1, n):
        src = lax.rem(me + n - d, n)
        remote(
            info, infos.at[src], info_send.at[d], info_recv.at[src], f, m, 1 - s
        ).wait_recv()

    all_states = states[...].astype(jnp.float32).reshape(total, width_d).astype(jnp.bfloat16)
    logits = lax.dot_general(
        all_states, embed[...], (((1,), (0,)), ((), ())), preferred_element_type=jnp.float32
    )
    capped = CAP * jnp.tanh(logits / CAP)
    rows = jnp.concatenate(
        [infos[b * nm * 2 + h] for b in range(nf) for h in (0, 1)], axis=0
    )
    ids = me * vocab + lax.broadcasted_iota(jnp.int32, (total, vocab), 1)
    hits = rows[:, 0:1] == ids
    e = jnp.sum(jnp.exp(capped), axis=1, keepdims=True)
    t = jnp.sum(jnp.where(hits, capped, 0.0), axis=1, keepdims=True)
    counted = rows[:, 64:65].astype(jnp.float32)
    lane = lax.broadcasted_iota(jnp.int32, (total, 128), 1)
    table = jnp.where(lane == 0, e, jnp.where(lane == 1, t, jnp.where(lane == 2, counted, 0.0)))
    pad = sums.shape[2]
    if pad > total:
        table = jnp.concatenate([table, jnp.zeros((pad - total, 128), jnp.float32)], axis=0)
    mine = jnp.transpose(table)[0:8, :]
    sums[me] = mine
    for d in range(1, n):
        pf, pm, ps = where_is(lax.rem(me + d, n))
        copy = remote(sums.at[me], sums.at[me], sum_send.at[d], sum_recv.at[me], pf, pm, ps)
        copy.start()
        pending.append(copy)
    for d in range(1, n):
        src = lax.rem(me + n - d, n)
        remote(
            sums.at[src], sums.at[src], sum_send.at[d], sum_recv.at[src], f, m, 1 - s
        ).wait_recv()
    added = jnp.sum(sums[...], axis=0)
    weights = mine[2:3, :]
    spot = lax.broadcasted_iota(jnp.int32, (1, pad), 1)
    exp_sums = jnp.where(spot < total, added[0:1, :], 1.0)
    losses = weights * (jnp.log(exp_sums) - added[1:2, :])
    mean = jnp.sum(losses, axis=1, keepdims=True) / jnp.maximum(
        jnp.sum(weights, axis=1, keepdims=True), 1.0
    )
    start = (f * 2 + s) * tok
    out[...] = pltpu.roll(losses, lax.rem(pad - start, pad), 1)[0, 0:tok]
    mean_out[...] = mean[0]

    swap.wait_send()
    swap_acc.wait_send()
    for copy in pending:
        copy.wait_send()
    for j in range(nf // nm):
        target, copy = to_owner(j)

        @pl.when(target != f)
        def _():
            copy.wait_send()

    @pl.when(owner)
    def _():
        for copy in state_sends():
            copy.wait_send()


def on_device(
    nf, nm, hidden, residual, down_packed, down_scale, post_gain, final_gain, embed_packed, embed_scale,
    targets, loss_mask,
):
    tok, width_d = residual.shape
    rows, cols = down_packed.shape
    vocab, packed = embed_packed.shape
    half = rows // 2
    n = nf * nm * 2
    total = tok * 2 * nf
    pad = -(-total // 128) * 128
    chunk = PLANES * (128 if half % 128 == 0 else half)
    vm = pl.BlockSpec(memory_space=pltpu.VMEM)
    hbm = pl.BlockSpec(memory_space=pl.ANY)
    sm = pl.BlockSpec(memory_space=pltpu.SMEM)
    dma = pltpu.SemaphoreType.DMA
    bf16, f32, i32 = jnp.bfloat16, jnp.float32, jnp.int32
    return pl.pallas_call(
        functools.partial(kernel, nf, nm),
        out_shape=(jax.ShapeDtypeStruct((tok,), f32), jax.ShapeDtypeStruct((1,), f32)),
        in_specs=[vm, vm, hbm, vm, vm, vm, hbm, vm, sm, sm],
        out_specs=(vm, vm),
        scratch_shapes=[
            pltpu.VMEM((half, cols), i32),
            pltpu.VMEM(down_scale.shape, f32),
            pltpu.VMEM((PLANES, half, cols), bf16),
            pltpu.VMEM((chunk, chunk), bf16),
            pltpu.VMEM((2, tok, half * PLANES), bf16),
            pltpu.VMEM((nf, PLANES, 2 * tok, half), bf16),
            pltpu.VMEM((2, nf, tok, cols), f32),
            pltpu.VMEM((nf, tok, cols), f32),
            pltpu.VMEM((nm, nf // nm, tok, cols), f32),
            pltpu.VMEM((nm, nf // nm, tok, cols), f32),
            pltpu.VMEM((nf // nm, tok, cols), f32),
            pltpu.VMEM((nf, tok, cols), f32),
            pltpu.VMEM((packed, vocab), i32),
            pltpu.VMEM((embed_scale.shape[1], vocab), f32),
            pltpu.VMEM((width_d, vocab), bf16),
            pltpu.VMEM((nf, 2, tok, width_d), bf16),
            pltpu.VMEM((tok, 128), i32),
            pltpu.VMEM((n, tok, 128), i32),
            pltpu.VMEM((n, 8, pad), f32),
            dma((2,)),
            dma, dma,
            dma((2, max(nf // 2, 1), PLANES)), dma((nf, PLANES)),
            dma((n,)), dma((n,)),
            dma((2,)),
            dma((nm,)), dma((nm,)),
            dma((nf // nm,)), dma((nf,)),
            dma((nf * nm,)), dma((nf,)),
            dma((nf,)), dma((nf,)),
            dma((n,)), dma((n,)),
        ],
        compiler_params=pltpu.CompilerParams(
            collective_id=0, has_side_effects=True, vmem_limit_bytes=62 * 1024 * 1024
        ),
    )(
        hidden, residual, down_packed, down_scale, post_gain, final_gain,
        embed_packed.T, embed_scale.T, targets, loss_mask,
    )


def solution(mesh):
    nf, nm = mesh.shape["fsdp"], mesh.shape["mp"]
    return jax.shard_map(
        functools.partial(on_device, nf, nm),
        mesh=mesh,
        in_specs=(
            P(("groups", "fsdp", "sub"), "mp"),
            P(("groups", "fsdp", "sub"), None),
            P("mp", "fsdp"),
            P("mp", "fsdp"),
            P(),
            P(),
            P(("fsdp", "mp", "sub"), None),
            P(("fsdp", "mp", "sub"), None),
            P(("groups", "fsdp", "sub")),
            P(("groups", "fsdp", "sub")),
        ),
        out_specs=(P(("groups", "fsdp", "sub")), P("groups")),
        check_vma=False,
    )
```

```python
import functools

import jax
import jax.numpy as jnp
from jax import lax
from jax.experimental import pallas as pl
from jax.experimental.pallas import tpu as pltpu
from jax.sharding import PartitionSpec as P

EPS = 1e-06
CAP = 30.0
MESH = pl.DeviceIdType.MESH
PLANES = 8
EARLY = 0.6


def remote(src, dst, send, recv, f, m, s):
    return pltpu.make_async_remote_copy(
        src_ref=src,
        dst_ref=dst,
        send_sem=send,
        recv_sem=recv,
        device_id={"fsdp": f, "mp": m, "sub": s},
        device_id_type=MESH,
    )


def kernel(
    nf, nm, hidden, residual, words_hbm, scale, post_gain, final_gain, embed_hbm, embed_scale, targets, mask,
    out, mean_out, words, scale_f, weight, perm, sorted_own, gathered, own_acc, acc_in, mid, mid_in, red, cols_in,
    embed_words, embed_f, embed, states, info, infos, sums,
    local_sem, pair_send, pair_recv, first_send, ring_send, ring_recv, info_send, info_recv,
    acc_sem, mid_send, mid_recv, col_send, col_recv, st_send, st_recv, side_send, fwd_send, fwd_recv,
    sum_send, sum_recv,
):
    f, m, s = lax.axis_index("fsdp"), lax.axis_index("mp"), lax.axis_index("sub")
    n = nf * nm * 2
    me = (f * nm + m) * 2 + s
    tok = hidden.shape[0]
    half_rows, cols = words.shape
    half_k = half_rows * PLANES
    total = tok * 2 * nf

    def where_is(q):
        return q // (2 * nm), (q // 2) % nm, q % 2

    load_words = pltpu.make_async_copy(
        words_hbm.at[pl.ds(pl.multiple_of(s * half_rows, 8), half_rows)], words, local_sem.at[0]
    )
    load_words.start()
    load_embed = pltpu.make_async_copy(embed_hbm, embed_words, local_sem.at[1])
    load_embed.start()

    barrier = pltpu.get_barrier_semaphore()
    for d in range(1, n):
        pf, pm, ps = where_is(lax.rem(me + d, n))
        pl.semaphore_signal(
            barrier, inc=1, device_id={"fsdp": pf, "mp": pm, "sub": ps}, device_id_type=MESH
        )

    width = perm.shape[0]
    q = width // PLANES
    step_rows = 128 if width % 128 == 0 else width

    col = lax.broadcasted_iota(jnp.int32, (1, width), 1)
    plane = sum(((col >= q * k).astype(jnp.int32) for k in range(1, PLANES)), jnp.zeros_like(col))
    source = (col - plane * q) * PLANES + plane

    def build(i, carry):
        start = pl.multiple_of(i * step_rows, step_rows)
        row = lax.broadcasted_iota(jnp.int32, (step_rows, width), 0)
        perm[pl.ds(start, step_rows), :] = jnp.where(row == source - start, 1.0, 0.0).astype(
            jnp.bfloat16
        )
        return carry

    lax.fori_loop(0, width // step_rows, build, 0)
    scale_f[...] = scale[...].astype(jnp.float32)
    own = hidden[...].astype(jnp.float32)
    chunks = half_k // width
    stacked = jnp.concatenate(
        [own[:, c * width:(c + 1) * width] for c in range(2 * chunks)], axis=0
    ).astype(jnp.bfloat16)
    ordered = jnp.dot(stacked, perm[...], preferred_element_type=jnp.float32)
    for c in range(2 * chunks):
        at = (c % chunks) * q
        for k in range(PLANES):
            sorted_own[c // chunks, k, :, at:at + q] = ordered[
                c * tok:(c + 1) * tok, k * q:(k + 1) * q
            ].astype(jnp.bfloat16)
    embed_f[...] = embed_scale[...].astype(jnp.float32)
    token = lax.broadcasted_iota(jnp.int32, (tok, 128), 0)
    side = lax.broadcasted_iota(jnp.int32, (tok, 128), 1)
    entry = jnp.zeros((tok, 128), jnp.int32)
    for i in range(tok):
        entry = jnp.where(token == i, jnp.where(side < 64, targets[i], mask[i]), entry)
    info[...] = entry
    infos[me] = entry
    gathered[f, :, s] = sorted_own[s]

    pl.semaphore_wait(barrier, n - 1)

    far = nf // 2
    low, high = list(range(4)), list(range(4, 8))
    orders = (low + high, high + low)
    last = (low, high)
    pending = []
    waited = set()

    def block_at(way, j):
        return lax.rem(f - j + nf, nf) if way == 0 else lax.rem(f + j, nf)

    def hop(way, j, p):
        slot = block_at(way, j - 1)
        target = lax.rem(f + 1, nf) if way == 0 else lax.rem(f + nf - 1, nf)
        return remote(
            gathered.at[slot, p], gathered.at[slot, p], ring_send.at[way, j - 1, p],
            ring_recv.at[slot, p, 0], target, m, s,
        )

    def send_hop(way, j, p):
        if j == 1 and (j < far or p in last[way]):
            target = lax.rem(f + 1, nf) if way == 0 else lax.rem(f + nf - 1, nf)
            for h in (0, 1):
                copy = remote(
                    sorted_own.at[h, p], gathered.at[f, p, s], first_send.at[way, p, h],
                    ring_recv.at[f, p, s], target, m, h,
                )
                copy.start()
                pending.append(copy)
        elif j < far or p in last[way]:
            copy = hop(way, j, p)
            copy.start()
            pending.append(copy)

    def arrive(way, j, p):
        if (way, j, p) in waited or not (j < far or p in last[way]):
            return
        waited.add((way, j, p))
        slot = block_at(way, j)
        if j == 1:
            for h in (0, 1):
                remote(
                    sorted_own.at[h, p], gathered.at[slot, p, h], first_send.at[way, p, h],
                    ring_recv.at[slot, p, h], f, m, 1 - s,
                ).wait_recv()
        else:
            remote(
                gathered.at[slot, p], gathered.at[slot, p], ring_send.at[way, j - 1, p],
                ring_recv.at[slot, p, 0], f, m, 1 - s,
            ).wait_recv()

    if nf > 1:
        for i in range(PLANES):
            for way in (0, 1):
                send_hop(way, 1, orders[way][i])

    swap = remote(
        sorted_own.at[1 - s], gathered.at[f, :, s], pair_send, pair_recv, f, m, 1 - s
    )
    swap.start()
    for d in range(1, n):
        peer = lax.rem(me + d, n)
        pf, pm, ps = where_is(peer)
        copy = remote(info, infos.at[me], info_send.at[d], info_recv.at[me], pf, pm, ps)
        copy.start()
        pending.append(copy)

    load_words.wait()
    per = half_rows // (scale.shape[0] // 2)
    groups = half_rows // per

    def dequant(i, carry):
        start = pl.multiple_of(i * per, per)
        w = words[pl.ds(start, per), :]
        sc = scale_f[pl.ds(s * groups + i, 1), :]
        for k in range(PLANES):
            code = jnp.right_shift(jnp.left_shift(w, 28 - 4 * k), 28) if k < 7 else jnp.right_shift(w, 28)
            weight[k, pl.ds(start, per), :] = (code.astype(jnp.float32) * sc).astype(jnp.bfloat16)
        return carry

    early = int(groups * EARLY)
    lax.fori_loop(0, early, dequant, 0)
    for j in range(1, far):
        for i in range(PLANES):
            for way in (0, 1):
                p = orders[way][i]
                if j + 1 < far or p in last[way]:
                    arrive(way, j, p)
                    send_hop(way, j + 1, p)
    lax.fori_loop(early, groups, dequant, 0)

    load_embed.wait()
    packed, vocab = embed_words.shape
    span = packed * PLANES // embed_f.shape[0]
    step = 32
    blocks = packed // step

    def dequant_embed(i, carry):
        w = embed_words[pl.ds(pl.multiple_of(i * step, step), step), :]
        for k in range(PLANES):
            code = jnp.right_shift(jnp.left_shift(w, 28 - 4 * k), 28) if k < 7 else jnp.right_shift(w, 28)
            sc = embed_f[pl.ds((k * packed + i * step) // span, 1), :]
            embed[pl.ds(pl.multiple_of(k * packed + i * step, step), step), :] = (
                code.astype(jnp.float32) * sc
            ).astype(jnp.bfloat16)
        return carry

    lax.fori_loop(0, blocks, dequant_embed, 0)

    for d in range(1, n):
        src = lax.rem(me + n - d, n)
        remote(
            info, infos.at[src], info_send.at[d], info_recv.at[src], f, m, 1 - s
        ).wait_recv()

    rows = jnp.concatenate(
        [infos[b * nm * 2 + h] for b in range(nf) for h in (0, 1)], axis=0
    )
    counted = jnp.broadcast_to(rows[:, 64:65].astype(jnp.float32), (total, 128))
    weights = jnp.transpose(
        jnp.concatenate([counted, jnp.zeros((total, 128), jnp.float32)], axis=0)
    )[0:1, :]

    swap.wait_recv()
    acc = jnp.zeros((total, cols), jnp.float32)
    for p in (0, 4, 1, 5, 2, 6, 3, 7):
        for j in range(1, far + 1):
            for way in (0, 1):
                arrive(way, j, p)
        lhs = gathered[:, p].astype(jnp.float32).reshape(total, half_rows).astype(jnp.bfloat16)
        acc = acc + jnp.dot(lhs, weight[p], preferred_element_type=jnp.float32)

    for b in range(nf):
        for h in (0, 1):
            r = (2 * b + h) * tok
            own_acc[h, b] = acc[r:r + tok]

    swap_acc = remote(own_acc.at[1 - s], acc_in, acc_sem.at[0], acc_sem.at[1], f, m, 1 - s)
    swap_acc.start()
    swap_acc.wait_recv()
    for b in range(nf):
        mid[b % nm, b // nm] = own_acc[s, b] + acc_in[b]
    for d in range(1, nm):
        pm = lax.rem(m + d, nm)
        copy = remote(mid.at[pm], mid_in.at[m], mid_send.at[d], mid_recv.at[m], f, pm, s)
        copy.start()
        pending.append(copy)
    part = mid[m]
    for d in range(1, nm):
        pm = lax.rem(m + d, nm)
        remote(mid.at[m], mid_in.at[pm], mid_send.at[0], mid_recv.at[pm], f, pm, s).wait_recv()
        part = part + mid_in[pm]
    red[...] = part

    def to_owner(j):
        target = j * nm + m
        return target, remote(
            red.at[j], cols_in.at[f], col_send.at[j], col_recv.at[f], target, m, s
        )

    for j in range(nf // nm):
        target, copy = to_owner(j)

        @pl.when(target != f)
        def _():
            copy.start()

        @pl.when(target == f)
        def _():
            cols_in[f] = red[j]

    owner = lax.rem(f, nm) == m

    def state_sends():
        return [
            remote(
                states.at[f, s], states.at[f, s], st_send.at[df], st_recv.at[f],
                lax.rem(f + df, nf), m, s,
            )
            for df in range(nf - 1, 0, -1)
        ]

    width_d = nf * cols

    @pl.when(owner)
    def _():
        for d in range(1, nf):
            src = lax.rem(f + d, nf)
            remote(
                red.at[0], cols_in.at[src], col_send.at[0], col_recv.at[src], src, m, s
            ).wait_recv()
        ffn = jnp.concatenate([cols_in[b] for b in range(nf)], axis=1)
        inv = lax.rsqrt(jnp.sum(ffn * ffn, axis=1, keepdims=True) / width_d + EPS)
        stream = residual[...].astype(jnp.float32) + ffn * inv * post_gain[...].reshape(1, width_d)
        inv2 = lax.rsqrt(jnp.sum(stream * stream, axis=1, keepdims=True) / width_d + EPS)
        states[f, s] = (stream * inv2 * final_gain[...].reshape(1, width_d)).astype(jnp.bfloat16)
        for copy in state_sends():
            copy.start()

    def forward(b):
        return remote(
            states.at[b, s], states.at[b, s], fwd_send.at[b], fwd_recv.at[b], f, m, 1 - s
        )

    for dm in range(nm):
        for j in range(nf // nm):
            b = j * nm + lax.rem(m + dm, nm)
            got = remote(
                states.at[b, s], states.at[b, s], st_send.at[0], st_recv.at[b], f, m, 1 - s
            )
            if dm == 0:
                @pl.when(b != f)
                def _():
                    got.wait_recv()

                for side in range(1, nm):
                    copy = remote(
                        states.at[b, s], states.at[b, s], side_send.at[j, side], st_recv.at[b],
                        f, lax.rem(m + side, nm), s,
                    )
                    copy.start()
                    pending.append(copy)
            else:
                got.wait_recv()
            copy = forward(b)
            copy.start()
            pending.append(copy)
    for b in range(nf):
        remote(
            states.at[b, 1 - s], states.at[b, 1 - s], fwd_send.at[b], fwd_recv.at[b], f, m, 1 - s
        ).wait_recv()
    all_states = states[...].astype(jnp.float32).reshape(total, width_d).astype(jnp.bfloat16)
    logits = lax.dot_general(
        all_states, embed[...], (((1,), (0,)), ((), ())), preferred_element_type=jnp.float32
    )
    capped = CAP * jnp.tanh(logits / CAP)
    ids = me * vocab + lax.broadcasted_iota(jnp.int32, (total, vocab), 1)
    hits = rows[:, 0:1] == ids
    e = jnp.sum(jnp.exp(capped), axis=1, keepdims=True)
    t = jnp.sum(jnp.where(hits, capped, 0.0), axis=1, keepdims=True)
    both = jnp.concatenate(
        [jnp.broadcast_to(e, (total, 128)), jnp.broadcast_to(t, (total, 128))], axis=0
    )
    sums[me] = jnp.transpose(both)[0:1, :]
    for d in range(1, n):
        pf, pm, ps = where_is(lax.rem(me + d, n))
        copy = remote(sums.at[me], sums.at[me], sum_send.at[d], sum_recv.at[me], pf, pm, ps)
        copy.start()
        pending.append(copy)
    for d in range(1, n):
        src = lax.rem(me + n - d, n)
        remote(
            sums.at[src], sums.at[src], sum_send.at[d], sum_recv.at[src], f, m, 1 - s
        ).wait_recv()
    added = jnp.sum(sums[...], axis=0)
    pad = 2 * total
    spot = lax.broadcasted_iota(jnp.int32, (1, pad), 1)
    exp_sums = jnp.where(spot < total, added, 1.0)
    losses = weights * (jnp.log(exp_sums) - pltpu.roll(added, total, 1))
    mean = jnp.sum(losses, axis=1, keepdims=True) / jnp.maximum(
        jnp.sum(weights, axis=1, keepdims=True), 1.0
    )
    start = (f * 2 + s) * tok
    out[...] = pltpu.roll(losses, lax.rem(pad - start, pad), 1)[0, 0:tok]
    mean_out[...] = mean[0]

    swap.wait_send()
    swap_acc.wait_send()
    for copy in pending:
        copy.wait_send()
    for j in range(nf // nm):
        target, copy = to_owner(j)

        @pl.when(target != f)
        def _():
            copy.wait_send()

    @pl.when(owner)
    def _():
        for copy in state_sends():
            copy.wait_send()


def on_device(
    nf, nm, hidden, residual, down_packed, down_scale, post_gain, final_gain, embed_packed, embed_scale,
    targets, loss_mask,
):
    tok, width_d = residual.shape
    rows, cols = down_packed.shape
    vocab, packed = embed_packed.shape
    half = rows // 2
    n = nf * nm * 2
    total = tok * 2 * nf
    chunk = PLANES * (128 if half % 128 == 0 else half)
    vm = pl.BlockSpec(memory_space=pltpu.VMEM)
    hbm = pl.BlockSpec(memory_space=pl.ANY)
    sm = pl.BlockSpec(memory_space=pltpu.SMEM)
    dma = pltpu.SemaphoreType.DMA
    bf16, f32, i32 = jnp.bfloat16, jnp.float32, jnp.int32
    return pl.pallas_call(
        functools.partial(kernel, nf, nm),
        out_shape=(jax.ShapeDtypeStruct((tok,), f32), jax.ShapeDtypeStruct((1,), f32)),
        in_specs=[vm, vm, hbm, vm, vm, vm, hbm, vm, sm, sm],
        out_specs=(vm, vm),
        scratch_shapes=[
            pltpu.VMEM((half, cols), i32),
            pltpu.VMEM(down_scale.shape, f32),
            pltpu.VMEM((PLANES, half, cols), bf16),
            pltpu.VMEM((chunk, chunk), bf16),
            pltpu.VMEM((2, PLANES, tok, half), bf16),
            pltpu.VMEM((nf, PLANES, 2, tok, half), bf16),
            pltpu.VMEM((2, nf, tok, cols), f32),
            pltpu.VMEM((nf, tok, cols), f32),
            pltpu.VMEM((nm, nf // nm, tok, cols), f32),
            pltpu.VMEM((nm, nf // nm, tok, cols), f32),
            pltpu.VMEM((nf // nm, tok, cols), f32),
            pltpu.VMEM((nf, tok, cols), f32),
            pltpu.VMEM((packed, vocab), i32),
            pltpu.VMEM((embed_scale.shape[1], vocab), f32),
            pltpu.VMEM((width_d, vocab), bf16),
            pltpu.VMEM((nf, 2, tok, width_d), bf16),
            pltpu.VMEM((tok, 128), i32),
            pltpu.VMEM((n, tok, 128), i32),
            pltpu.VMEM((n, 1, 2 * total), f32),
            dma((2,)),
            dma, dma,
            dma((2, PLANES, 2)), dma((2, max(nf // 2, 1), PLANES)), dma((nf, PLANES, 2)),
            dma((n,)), dma((n,)),
            dma((2,)),
            dma((nm,)), dma((nm,)),
            dma((nf // nm,)), dma((nf,)),
            dma((nf,)), dma((nf,)), dma((nf // nm, nm)),
            dma((nf,)), dma((nf,)),
            dma((n,)), dma((n,)),
        ],
        compiler_params=pltpu.CompilerParams(
            collective_id=0, has_side_effects=True, vmem_limit_bytes=62 * 1024 * 1024
        ),
    )(
        hidden, residual, down_packed, down_scale, post_gain, final_gain,
        embed_packed.T, embed_scale.T, targets, loss_mask,
    )


def solution(mesh):
    nf, nm = mesh.shape["fsdp"], mesh.shape["mp"]
    return jax.shard_map(
        functools.partial(on_device, nf, nm),
        mesh=mesh,
        in_specs=(
            P(("groups", "fsdp", "sub"), "mp"),
            P(("groups", "fsdp", "sub"), None),
            P("mp", "fsdp"),
            P("mp", "fsdp"),
            P(),
            P(),
            P(("fsdp", "mp", "sub"), None),
            P(("fsdp", "mp", "sub"), None),
            P(("groups", "fsdp", "sub")),
            P(("groups", "fsdp", "sub")),
        ),
        out_specs=(P(("groups", "fsdp", "sub")), P("groups")),
        check_vma=False,
    )
```

```python
import functools

import jax
import jax.numpy as jnp
from jax import lax
from jax.experimental import pallas as pl
from jax.experimental.pallas import tpu as pltpu
from jax.sharding import PartitionSpec as P

EPS = 1e-06
CAP = 30.0
MESH = pl.DeviceIdType.MESH
PLANES = 8
EARLY = 0.6
PIECES = 2


def remote(src, dst, send, recv, f, m, s):
    return pltpu.make_async_remote_copy(
        src_ref=src,
        dst_ref=dst,
        send_sem=send,
        recv_sem=recv,
        device_id={"fsdp": f, "mp": m, "sub": s},
        device_id_type=MESH,
    )


def kernel(
    nf, nm, hidden, residual, words_hbm, scale, post_gain, final_gain, embed_hbm, embed_scale, targets, mask,
    out, mean_out, words, scale_f, weight, perm, sorted_own, gathered, own_acc, acc_in, mid, mid_in, red, cols_in,
    embed_words, embed_f, embed, states, info, infos, sums,
    local_sem, pair_send, pair_recv, first_send, ring_send, ring_recv, info_send, info_recv,
    acc_sem, mid_send, mid_recv, col_send, col_recv, st_send, st_recv, side_send, fwd_send, fwd_recv,
    sum_send, sum_recv,
):
    f, m, s = lax.axis_index("fsdp"), lax.axis_index("mp"), lax.axis_index("sub")
    n = nf * nm * 2
    me = (f * nm + m) * 2 + s
    tok = hidden.shape[0]
    half_rows, cols = words.shape
    half_k = half_rows * PLANES
    total = tok * 2 * nf

    def where_is(q):
        return q // (2 * nm), (q // 2) % nm, q % 2

    load_words = pltpu.make_async_copy(
        words_hbm.at[pl.ds(pl.multiple_of(s * half_rows, 8), half_rows)], words, local_sem.at[0]
    )
    load_words.start()
    load_embed = pltpu.make_async_copy(embed_hbm, embed_words, local_sem.at[1])
    load_embed.start()

    barrier = pltpu.get_barrier_semaphore()
    for d in range(1, n):
        pf, pm, ps = where_is(lax.rem(me + d, n))
        pl.semaphore_signal(
            barrier, inc=1, device_id={"fsdp": pf, "mp": pm, "sub": ps}, device_id_type=MESH
        )

    width = perm.shape[0]
    q = width // PLANES
    step_rows = 128 if width % 128 == 0 else width

    col = lax.broadcasted_iota(jnp.int32, (1, width), 1)
    plane = sum(((col >= q * k).astype(jnp.int32) for k in range(1, PLANES)), jnp.zeros_like(col))
    source = (col - plane * q) * PLANES + plane

    def build(i, carry):
        start = pl.multiple_of(i * step_rows, step_rows)
        row = lax.broadcasted_iota(jnp.int32, (step_rows, width), 0)
        perm[pl.ds(start, step_rows), :] = jnp.where(row == source - start, 1.0, 0.0).astype(
            jnp.bfloat16
        )
        return carry

    lax.fori_loop(0, width // step_rows, build, 0)
    scale_f[...] = scale[...].astype(jnp.float32)
    own = hidden[...].astype(jnp.float32)
    chunks = half_k // width
    stacked = jnp.concatenate(
        [own[:, c * width:(c + 1) * width] for c in range(2 * chunks)], axis=0
    ).astype(jnp.bfloat16)
    ordered = jnp.dot(stacked, perm[...], preferred_element_type=jnp.float32)
    for c in range(2 * chunks):
        at = (c % chunks) * q
        for k in range(PLANES):
            sorted_own[c // chunks, k, :, at:at + q] = ordered[
                c * tok:(c + 1) * tok, k * q:(k + 1) * q
            ].astype(jnp.bfloat16)
    embed_f[...] = embed_scale[...].astype(jnp.float32)
    token = lax.broadcasted_iota(jnp.int32, (tok, 128), 0)
    side = lax.broadcasted_iota(jnp.int32, (tok, 128), 1)
    entry = jnp.zeros((tok, 128), jnp.int32)
    for i in range(tok):
        entry = jnp.where(token == i, jnp.where(side < 64, targets[i], mask[i]), entry)
    info[...] = entry
    infos[me] = entry
    gathered[f, :, s] = sorted_own[s]

    pl.semaphore_wait(barrier, n - 1)

    far = nf // 2
    low, high = list(range(4)), list(range(4, 8))
    orders = (low + high, high + low)
    last = (low, high)
    pending = []
    waited = set()

    def block_at(way, j):
        return lax.rem(f - j + nf, nf) if way == 0 else lax.rem(f + j, nf)

    def hop(way, j, p):
        slot = block_at(way, j - 1)
        target = lax.rem(f + 1, nf) if way == 0 else lax.rem(f + nf - 1, nf)
        return remote(
            gathered.at[slot, p], gathered.at[slot, p], ring_send.at[way, j - 1, p],
            ring_recv.at[slot, p, 0], target, m, s,
        )

    def send_hop(way, j, p):
        if j == 1 and (j < far or p in last[way]):
            target = lax.rem(f + 1, nf) if way == 0 else lax.rem(f + nf - 1, nf)
            for h in (0, 1):
                copy = remote(
                    sorted_own.at[h, p], gathered.at[f, p, s], first_send.at[way, p, h],
                    ring_recv.at[f, p, s], target, m, h,
                )
                copy.start()
                pending.append(copy)
        elif j < far or p in last[way]:
            copy = hop(way, j, p)
            copy.start()
            pending.append(copy)

    def arrive(way, j, p):
        if (way, j, p) in waited or not (j < far or p in last[way]):
            return
        waited.add((way, j, p))
        slot = block_at(way, j)
        if j == 1:
            for h in (0, 1):
                remote(
                    sorted_own.at[h, p], gathered.at[slot, p, h], first_send.at[way, p, h],
                    ring_recv.at[slot, p, h], f, m, 1 - s,
                ).wait_recv()
        else:
            remote(
                gathered.at[slot, p], gathered.at[slot, p], ring_send.at[way, j - 1, p],
                ring_recv.at[slot, p, 0], f, m, 1 - s,
            ).wait_recv()

    if nf > 1:
        for i in range(PLANES):
            for way in (0, 1):
                send_hop(way, 1, orders[way][i])

    swap = remote(
        sorted_own.at[1 - s], gathered.at[f, :, s], pair_send, pair_recv, f, m, 1 - s
    )
    swap.start()
    for d in range(1, n):
        peer = lax.rem(me + d, n)
        pf, pm, ps = where_is(peer)
        copy = remote(info, infos.at[me], info_send.at[d], info_recv.at[me], pf, pm, ps)
        copy.start()
        pending.append(copy)

    load_words.wait()
    per = half_rows // (scale.shape[0] // 2)
    groups = half_rows // per

    def dequant(i, carry):
        start = pl.multiple_of(i * per, per)
        w = words[pl.ds(start, per), :]
        sc = scale_f[pl.ds(s * groups + i, 1), :]
        for k in range(PLANES):
            code = jnp.right_shift(jnp.left_shift(w, 28 - 4 * k), 28) if k < 7 else jnp.right_shift(w, 28)
            weight[k, pl.ds(start, per), :] = (code.astype(jnp.float32) * sc).astype(jnp.bfloat16)
        return carry

    early = int(groups * EARLY)
    lax.fori_loop(0, early, dequant, 0)
    for j in range(1, far):
        for i in range(PLANES):
            for way in (0, 1):
                p = orders[way][i]
                if j + 1 < far or p in last[way]:
                    arrive(way, j, p)
                    send_hop(way, j + 1, p)
    lax.fori_loop(early, groups, dequant, 0)

    load_embed.wait()
    packed, vocab = embed_words.shape
    span = packed * PLANES // embed_f.shape[0]
    step = 32
    blocks = packed // step

    def dequant_embed(i, carry):
        w = embed_words[pl.ds(pl.multiple_of(i * step, step), step), :]
        for k in range(PLANES):
            code = jnp.right_shift(jnp.left_shift(w, 28 - 4 * k), 28) if k < 7 else jnp.right_shift(w, 28)
            sc = embed_f[pl.ds((k * packed + i * step) // span, 1), :]
            embed[pl.ds(pl.multiple_of(k * packed + i * step, step), step), :] = (
                code.astype(jnp.float32) * sc
            ).astype(jnp.bfloat16)
        return carry

    lax.fori_loop(0, blocks, dequant_embed, 0)

    for d in range(1, n):
        src = lax.rem(me + n - d, n)
        remote(
            info, infos.at[src], info_send.at[d], info_recv.at[src], f, m, 1 - s
        ).wait_recv()

    rows = jnp.concatenate(
        [infos[b * nm * 2 + h] for b in range(nf) for h in (0, 1)], axis=0
    )
    counted = jnp.broadcast_to(rows[:, 64:65].astype(jnp.float32), (total, 128))
    weights = jnp.transpose(
        jnp.concatenate([counted, jnp.zeros((total, 128), jnp.float32)], axis=0)
    )[0:1, :]

    swap.wait_recv()
    acc = jnp.zeros((total, cols), jnp.float32)
    for p in (0, 4, 1, 5, 2, 6, 3, 7):
        for j in range(1, far + 1):
            for way in (0, 1):
                arrive(way, j, p)
        lhs = gathered[:, p].astype(jnp.float32).reshape(total, half_rows).astype(jnp.bfloat16)
        acc = acc + jnp.dot(lhs, weight[p], preferred_element_type=jnp.float32)

    for b in range(nf):
        for h in (0, 1):
            r = (2 * b + h) * tok
            own_acc[h, b] = acc[r:r + tok]

    swap_acc = remote(own_acc.at[1 - s], acc_in, acc_sem.at[0], acc_sem.at[1], f, m, 1 - s)
    swap_acc.start()
    swap_acc.wait_recv()
    for b in range(nf):
        mid[b % nm, b // nm] = own_acc[s, b] + acc_in[b]
    for d in range(1, nm):
        pm = lax.rem(m + d, nm)
        copy = remote(mid.at[pm], mid_in.at[m], mid_send.at[d], mid_recv.at[m], f, pm, s)
        copy.start()
        pending.append(copy)
    part = mid[m]
    for d in range(1, nm):
        pm = lax.rem(m + d, nm)
        remote(mid.at[m], mid_in.at[pm], mid_send.at[0], mid_recv.at[pm], f, pm, s).wait_recv()
        part = part + mid_in[pm]
    red[...] = part

    def to_owner(j):
        target = j * nm + m
        return target, remote(
            red.at[j], cols_in.at[f], col_send.at[j], col_recv.at[f], target, m, s
        )

    for j in range(nf // nm):
        target, copy = to_owner(j)

        @pl.when(target != f)
        def _():
            copy.start()

        @pl.when(target == f)
        def _():
            cols_in[f] = red[j]

    owner = lax.rem(f, nm) == m

    def state_sends():
        return [
            remote(
                states.at[h, f, s], states.at[h, f, s], st_send.at[h, df], st_recv.at[h, f],
                lax.rem(f + df, nf), m, s,
            )
            for h in range(PIECES)
            for df in range(nf - 1, 0, -1)
        ]

    width_d = nf * cols

    @pl.when(owner)
    def _():
        for d in range(1, nf):
            src = lax.rem(f + d, nf)
            remote(
                red.at[0], cols_in.at[src], col_send.at[0], col_recv.at[src], src, m, s
            ).wait_recv()
        ffn = jnp.concatenate([cols_in[b] for b in range(nf)], axis=1)
        inv = lax.rsqrt(jnp.sum(ffn * ffn, axis=1, keepdims=True) / width_d + EPS)
        stream = residual[...].astype(jnp.float32) + ffn * inv * post_gain[...].reshape(1, width_d)
        inv2 = lax.rsqrt(jnp.sum(stream * stream, axis=1, keepdims=True) / width_d + EPS)
        done = (stream * inv2 * final_gain[...].reshape(1, width_d)).astype(jnp.bfloat16)
        for h in range(PIECES):
            states[h, f, s] = done[:, h * (width_d // PIECES):(h + 1) * (width_d // PIECES)]
        for copy in state_sends():
            copy.start()

    def forward(h, b):
        return remote(
            states.at[h, b, s], states.at[h, b, s], fwd_send.at[h, b], fwd_recv.at[h, b],
            f, m, 1 - s,
        )

    for dm in range(nm):
        for h in range(PIECES):
            for j in range(nf // nm):
                b = j * nm + lax.rem(m + dm, nm)
                got = remote(
                    states.at[h, b, s], states.at[h, b, s], st_send.at[h, 0], st_recv.at[h, b],
                    f, m, 1 - s,
                )
                if dm == 0:
                    @pl.when(b != f)
                    def _():
                        got.wait_recv()

                    for side in range(1, nm):
                        copy = remote(
                            states.at[h, b, s], states.at[h, b, s], side_send.at[h, j, side],
                            st_recv.at[h, b], f, lax.rem(m + side, nm), s,
                        )
                        copy.start()
                        pending.append(copy)
                else:
                    got.wait_recv()
                copy = forward(h, b)
                copy.start()
                pending.append(copy)
    for h in range(PIECES):
        for b in range(nf):
            remote(
                states.at[h, b, 1 - s], states.at[h, b, 1 - s], fwd_send.at[h, b],
                fwd_recv.at[h, b], f, m, 1 - s,
            ).wait_recv()
    logits = jnp.zeros((total, vocab), jnp.float32)
    part_d = width_d // PIECES
    for h in range(PIECES):
        some = states[h].astype(jnp.float32).reshape(total, part_d).astype(jnp.bfloat16)
        logits = logits + jnp.dot(
            some, embed[h * part_d:(h + 1) * part_d, :], preferred_element_type=jnp.float32
        )
    capped = CAP * jnp.tanh(logits / CAP)
    ids = me * vocab + lax.broadcasted_iota(jnp.int32, (total, vocab), 1)
    hits = rows[:, 0:1] == ids
    e = jnp.sum(jnp.exp(capped), axis=1, keepdims=True)
    t = jnp.sum(jnp.where(hits, capped, 0.0), axis=1, keepdims=True)
    both = jnp.concatenate(
        [jnp.broadcast_to(e, (total, 128)), jnp.broadcast_to(t, (total, 128))], axis=0
    )
    sums[me] = jnp.transpose(both)[0:1, :]
    for d in range(1, n):
        pf, pm, ps = where_is(lax.rem(me + d, n))
        copy = remote(sums.at[me], sums.at[me], sum_send.at[d], sum_recv.at[me], pf, pm, ps)
        copy.start()
        pending.append(copy)
    for d in range(1, n):
        src = lax.rem(me + n - d, n)
        remote(
            sums.at[src], sums.at[src], sum_send.at[d], sum_recv.at[src], f, m, 1 - s
        ).wait_recv()
    added = jnp.sum(sums[...], axis=0)
    pad = 2 * total
    spot = lax.broadcasted_iota(jnp.int32, (1, pad), 1)
    exp_sums = jnp.where(spot < total, added, 1.0)
    losses = weights * (jnp.log(exp_sums) - pltpu.roll(added, total, 1))
    mean = jnp.sum(losses, axis=1, keepdims=True) / jnp.maximum(
        jnp.sum(weights, axis=1, keepdims=True), 1.0
    )
    start = (f * 2 + s) * tok
    out[...] = pltpu.roll(losses, lax.rem(pad - start, pad), 1)[0, 0:tok]
    mean_out[...] = mean[0]

    swap.wait_send()
    swap_acc.wait_send()
    for copy in pending:
        copy.wait_send()
    for j in range(nf // nm):
        target, copy = to_owner(j)

        @pl.when(target != f)
        def _():
            copy.wait_send()

    @pl.when(owner)
    def _():
        for copy in state_sends():
            copy.wait_send()


def on_device(
    nf, nm, hidden, residual, down_packed, down_scale, post_gain, final_gain, embed_packed, embed_scale,
    targets, loss_mask,
):
    tok, width_d = residual.shape
    rows, cols = down_packed.shape
    vocab, packed = embed_packed.shape
    half = rows // 2
    n = nf * nm * 2
    total = tok * 2 * nf
    chunk = PLANES * (128 if half % 128 == 0 else half)
    vm = pl.BlockSpec(memory_space=pltpu.VMEM)
    hbm = pl.BlockSpec(memory_space=pl.ANY)
    sm = pl.BlockSpec(memory_space=pltpu.SMEM)
    dma = pltpu.SemaphoreType.DMA
    bf16, f32, i32 = jnp.bfloat16, jnp.float32, jnp.int32
    return pl.pallas_call(
        functools.partial(kernel, nf, nm),
        out_shape=(jax.ShapeDtypeStruct((tok,), f32), jax.ShapeDtypeStruct((1,), f32)),
        in_specs=[vm, vm, hbm, vm, vm, vm, hbm, vm, sm, sm],
        out_specs=(vm, vm),
        scratch_shapes=[
            pltpu.VMEM((half, cols), i32),
            pltpu.VMEM(down_scale.shape, f32),
            pltpu.VMEM((PLANES, half, cols), bf16),
            pltpu.VMEM((chunk, chunk), bf16),
            pltpu.VMEM((2, PLANES, tok, half), bf16),
            pltpu.VMEM((nf, PLANES, 2, tok, half), bf16),
            pltpu.VMEM((2, nf, tok, cols), f32),
            pltpu.VMEM((nf, tok, cols), f32),
            pltpu.VMEM((nm, nf // nm, tok, cols), f32),
            pltpu.VMEM((nm, nf // nm, tok, cols), f32),
            pltpu.VMEM((nf // nm, tok, cols), f32),
            pltpu.VMEM((nf, tok, cols), f32),
            pltpu.VMEM((packed, vocab), i32),
            pltpu.VMEM((embed_scale.shape[1], vocab), f32),
            pltpu.VMEM((width_d, vocab), bf16),
            pltpu.VMEM((PIECES, nf, 2, tok, width_d // PIECES), bf16),
            pltpu.VMEM((tok, 128), i32),
            pltpu.VMEM((n, tok, 128), i32),
            pltpu.VMEM((n, 1, 2 * total), f32),
            dma((2,)),
            dma, dma,
            dma((2, PLANES, 2)), dma((2, max(nf // 2, 1), PLANES)), dma((nf, PLANES, 2)),
            dma((n,)), dma((n,)),
            dma((2,)),
            dma((nm,)), dma((nm,)),
            dma((nf // nm,)), dma((nf,)),
            dma((PIECES, nf)), dma((PIECES, nf)), dma((PIECES, nf // nm, nm)),
            dma((PIECES, nf)), dma((PIECES, nf)),
            dma((n,)), dma((n,)),
        ],
        compiler_params=pltpu.CompilerParams(
            collective_id=0, has_side_effects=True, vmem_limit_bytes=62 * 1024 * 1024
        ),
    )(
        hidden, residual, down_packed, down_scale, post_gain, final_gain,
        embed_packed.T, embed_scale.T, targets, loss_mask,
    )


def solution(mesh):
    nf, nm = mesh.shape["fsdp"], mesh.shape["mp"]
    return jax.shard_map(
        functools.partial(on_device, nf, nm),
        mesh=mesh,
        in_specs=(
            P(("groups", "fsdp", "sub"), "mp"),
            P(("groups", "fsdp", "sub"), None),
            P("mp", "fsdp"),
            P("mp", "fsdp"),
            P(),
            P(),
            P(("fsdp", "mp", "sub"), None),
            P(("fsdp", "mp", "sub"), None),
            P(("groups", "fsdp", "sub")),
            P(("groups", "fsdp", "sub")),
        ),
        out_specs=(P(("groups", "fsdp", "sub")), P("groups")),
        check_vma=False,
    )
```
